32 devices in a mesh: rep: 2 (over x), tp: 4 (over z), sp: 4 (over y, core).
Axes of the slice: x: 2, y: 2, z: 4, core: 2. Of those that a mesh axis runs over, the one named last changes fastest.
Arguments:
- x_in: bfloat16 [8192, 5376], P(('rep', 'sp')), parts along dimension 0
- positions: int32 [8192], P(('rep', 'sp')), parts along dimension 0
- segments: int32 [8192], P(('rep', 'sp')), parts along dimension 0
- gain_attn: float32 [5376], replicated
- w_q: bfloat16 [5376, 4096], P(None, 'tp')
- w_k: bfloat16 [5376, 2048], P(None, 'tp')
- w_v: bfloat16 [5376, 2048], P(None, 'tp')
- w_o: bfloat16 [4096, 5376], P('tp')
- gain_mlp: float32 [5376], replicated
- w_gate: bfloat16 [5376, 21504], P(None, 'tp')
- w_up: bfloat16 [5376, 21504], P(None, 'tp')
- w_down: bfloat16 [21504, 5376], P('tp')
Outputs:
- output 1: bfloat16 [8192, 5376], P(('rep', 'sp')), parts along dimension 0
- output 2: bfloat16 [8192, 16, 128], P('rep', ('tp', 'sp')), parts along dimension 0
- output 3: bfloat16 [8192, 16, 128], P('rep', ('tp', 'sp')), parts along dimension 0
There are 2 independent parts. The reference program is written for one: setup_inputs(seed, part) draws one part's arguments, and reference() takes and returns one part's arrays. A program takes and returns all parts, laid end to end along the dimension named above; an argument that names none is the same for every part.
All inputs are finite; a program needn't handle non-finite values.
Results may differ from the reference program's by a relative error of at most 0.00707664.
Values are sent between devices in bfloat16 or wider.
A program may use at most 1 GiB of HBM per device.

```python
import jax
import jax.numpy as jnp
from jax import lax

TOKENS = 4096
MODEL_DIM = 5376
FF_DIM = 21504
Q_HEADS = 32
KV_HEADS = 16
HEAD_DIM = 128
NUM_REQS = 2
KV_SLOTS = 16
ROPE_BASE = 500000
NORM_EPS = 1e-5


def draw_layout(layout_key):
    cut_key, step_key, start_key = jax.random.split(layout_key, 3)
    cut_rows = jnp.sort(jax.random.choice(cut_key, TOKENS - 1, (NUM_REQS - 1,), replace=False) + 1).astype(jnp.int32)
    tok_index = jnp.arange(TOKENS, dtype=jnp.int32)
    segments = jnp.sum(tok_index[:, None] >= cut_rows[None, :], axis=1).astype(jnp.int32)
    step_sizes = jax.random.randint(step_key, (TOKENS,), 1, 4, dtype=jnp.int32)
    run_sum = jnp.cumsum(step_sizes)
    first_rows = jnp.concatenate([jnp.zeros((1,), jnp.int32), cut_rows])
    seg_base = run_sum[first_rows] - step_sizes[first_rows]
    start_pos = jax.random.randint(start_key, (NUM_REQS,), 0, 1024, dtype=jnp.int32)
    positions = (run_sum - seg_base[segments] + start_pos[segments]).astype(jnp.int32)
    return positions, segments


def setup_inputs(seed: int = 0, part: int = 0) -> dict:
    base_key = jax.random.key(seed)
    part_key = jax.random.fold_in(base_key, part)
    x_key, layout_key = jax.random.split(part_key, 2)
    w_keys = jax.random.split(base_key, 10)
    positions, segments = draw_layout(layout_key)
    d_scale = MODEL_DIM ** -0.5

    def normal_weight(key_w, shape, std_dev):
        return (jax.random.normal(key_w, shape, jnp.float32) * std_dev).astype(jnp.bfloat16)

    return {
        "x_in": jax.random.normal(x_key, (TOKENS, MODEL_DIM), jnp.float32).astype(jnp.bfloat16),
        "positions": positions,
        "segments": segments,
        "gain_attn": 1.0 + 0.25 * jax.random.normal(w_keys[0], (MODEL_DIM,), jnp.float32),
        "w_q": normal_weight(w_keys[1], (MODEL_DIM, Q_HEADS * HEAD_DIM), 1.6 * d_scale),
        "w_k": normal_weight(w_keys[2], (MODEL_DIM, KV_HEADS * HEAD_DIM), 1.6 * d_scale),
        "w_v": normal_weight(w_keys[3], (MODEL_DIM, KV_HEADS * HEAD_DIM), d_scale),
        "w_o": normal_weight(w_keys[4], (Q_HEADS * HEAD_DIM, MODEL_DIM), (Q_HEADS * HEAD_DIM) ** -0.5),
        "gain_mlp": 1.0 + 0.25 * jax.random.normal(w_keys[5], (MODEL_DIM,), jnp.float32),
        "w_gate": normal_weight(w_keys[6], (MODEL_DIM, FF_DIM), d_scale),
        "w_up": normal_weight(w_keys[7], (MODEL_DIM, FF_DIM), d_scale),
        "w_down": normal_weight(w_keys[8], (FF_DIM, MODEL_DIM), FF_DIM ** -0.5),
    }


def rms_norm(x_f32, gain_vec):
    mean_sq = jnp.mean(x_f32 * x_f32, axis=-1, keepdims=True)
    return (x_f32 * lax.rsqrt(mean_sq + NORM_EPS) * gain_vec).astype(jnp.bfloat16)


def rope_tables(positions):
    half_dim = HEAD_DIM // 2
    inv_freq = jnp.power(jnp.float32(ROPE_BASE), -jnp.arange(half_dim, dtype=jnp.float32) * (2.0 / HEAD_DIM))
    angles = positions.astype(jnp.float32)[:, None] * inv_freq[None, :]
    return jnp.cos(angles)[:, None, :], jnp.sin(angles)[:, None, :]


def rotate(t_f32, cos_t, sin_t):
    half_dim = HEAD_DIM // 2
    t_lo = t_f32[..., :half_dim]
    t_hi = t_f32[..., half_dim:]
    return jnp.concatenate([t_lo * cos_t - t_hi * sin_t, t_hi * cos_t + t_lo * sin_t], axis=-1)


def reference(x_in, positions, segments, gain_attn, w_q, w_k, w_v, w_o, gain_mlp, w_gate, w_up, w_down):
    x_f32 = x_in.astype(jnp.float32)
    u_norm = rms_norm(x_f32, gain_attn)
    cos_t, sin_t = rope_tables(positions)
    q_rot = rotate(jnp.dot(u_norm, w_q, preferred_element_type=jnp.float32).reshape(TOKENS, Q_HEADS, HEAD_DIM), cos_t, sin_t).astype(jnp.bfloat16)
    k_rot = rotate(jnp.dot(u_norm, w_k, preferred_element_type=jnp.float32).reshape(TOKENS, KV_HEADS, HEAD_DIM), cos_t, sin_t).astype(jnp.bfloat16)
    v_proj = jnp.dot(u_norm, w_v, preferred_element_type=jnp.float32).astype(jnp.bfloat16).reshape(TOKENS, KV_HEADS, HEAD_DIM)
    group_size = Q_HEADS // KV_HEADS
    tok_index = jnp.arange(TOKENS)
    allowed = (tok_index[:, None] >= tok_index[None, :]) & (segments[:, None] == segments[None, :])
    score_scale = HEAD_DIM ** -0.5

    def one_head(operands):
        q_one, k_one, v_one = operands
        scores = jnp.dot(q_one, k_one.T, preferred_element_type=jnp.float32) * score_scale
        scores = jnp.where(allowed, scores, -1e30)
        prob_bf16 = jax.nn.softmax(scores, axis=-1).astype(jnp.bfloat16)
        return jnp.dot(prob_bf16, v_one, preferred_element_type=jnp.float32).astype(jnp.bfloat16)

    q_heads = jnp.transpose(q_rot, (1, 0, 2))
    k_heads = jnp.repeat(jnp.transpose(k_rot, (1, 0, 2)), group_size, axis=0)
    v_heads = jnp.repeat(jnp.transpose(v_proj, (1, 0, 2)), group_size, axis=0)
    attn_out = jnp.transpose(lax.map(one_head, (q_heads, k_heads, v_heads)), (1, 0, 2)).reshape(TOKENS, Q_HEADS * HEAD_DIM)
    x_mid = x_f32 + jnp.dot(attn_out, w_o, preferred_element_type=jnp.float32)
    u_mlp = rms_norm(x_mid, gain_mlp)
    gate_act = jnp.dot(u_mlp, w_gate, preferred_element_type=jnp.float32)
    up_act = jnp.dot(u_mlp, w_up, preferred_element_type=jnp.float32)
    hidden = (jax.nn.silu(gate_act) * up_act).astype(jnp.bfloat16)
    y_out = (x_mid + jnp.dot(hidden, w_down, preferred_element_type=jnp.float32)).astype(jnp.bfloat16)
    slot_repeat = KV_SLOTS // KV_HEADS
    return y_out, jnp.repeat(k_rot, slot_repeat, axis=1), jnp.repeat(v_proj, slot_repeat, axis=1)
```

```python
import functools
import jax
import jax.numpy as jnp
from jax import lax
from jax.experimental import pallas as pl
from jax.experimental.pallas import tpu as pltpu
from jax.sharding import PartitionSpec as P

HEAD_DIM = 128
ROPE_BASE = 500000.0
NORM_EPS = 1e-5
CHUNKS = (512, 512)
ATTN_ROWS = 256
SUB_ROWS = 64
KV_BLOCK = 512


def rms_norm(x_f32, gain_vec):
    mean_sq = jnp.mean(x_f32 * x_f32, axis=-1, keepdims=True)
    return (x_f32 * lax.rsqrt(mean_sq + NORM_EPS) * gain_vec).astype(jnp.bfloat16)


def rope_tables(positions):
    half_dim = HEAD_DIM // 2
    inv_freq = jnp.power(jnp.float32(ROPE_BASE), -jnp.arange(half_dim, dtype=jnp.float32) * (2.0 / HEAD_DIM))
    angles = positions.astype(jnp.float32)[:, None] * inv_freq
    return jnp.cos(angles), jnp.sin(angles)


def rotate_heads(t_f32, cos_t, sin_t):
    half_dim = HEAD_DIM // 2
    pieces = []
    for start in range(0, t_f32.shape[1], HEAD_DIM):
        t_lo = t_f32[:, start:start + half_dim]
        t_hi = t_f32[:, start + half_dim:start + HEAD_DIM]
        pieces += [t_lo * cos_t - t_hi * sin_t, t_hi * cos_t + t_lo * sin_t]
    return jnp.concatenate(pieces, axis=1).astype(jnp.bfloat16)


def attention_kernel(row_offset, row_stride, per_block, group, q_ref, k_ref, v_ref, segq_ref, segk_ref, o_ref, s_ref):
    rows = q_ref.shape[0]
    row_start = lax.div(pl.program_id(0), per_block) * row_stride + row_offset + lax.rem(pl.program_id(0), per_block) * rows
    n_blocks = lax.div(row_start + rows + KV_BLOCK - 1, KV_BLOCK)
    seg_q = segq_ref[...]
    row_ids = row_start + lax.broadcasted_iota(jnp.int32, (rows, KV_BLOCK), 0)
    lane_ids = lax.broadcasted_iota(jnp.int32, (rows, KV_BLOCK), 1)
    lanes = [slice(i, i + 128) for i in range(0, KV_BLOCK, 128)]

    def score_step(j, accs):
        cols = pl.ds(pl.multiple_of(j * KV_BLOCK, KV_BLOCK), KV_BLOCK)
        k_blk = k_ref[cols, :]
        allowed = (row_ids >= lane_ids + j * KV_BLOCK) & (seg_q == segk_ref[:, cols])
        out = []
        for g in range(group):
            scores = lax.dot_general(q_ref[:, g * HEAD_DIM:(g + 1) * HEAD_DIM], k_blk, (((1,), (1,)), ((), ())),
                                     preferred_element_type=jnp.float32) * (HEAD_DIM ** -0.5)
            scores = jnp.where(allowed, scores, -1e30)
            s_ref[g, :, cols] = scores
            acc = accs[g]
            for sl in lanes:
                acc = jnp.maximum(acc, scores[:, sl])
            out.append(acc)
        return tuple(out)

    accs = lax.fori_loop(0, n_blocks, score_step, tuple(jnp.full((rows, 128), -1e30, jnp.float32) for _ in range(group)))
    maxes = [jnp.max(a, axis=1, keepdims=True) for a in accs]

    def exp_step(j, accs):
        cols = pl.ds(pl.multiple_of(j * KV_BLOCK, KV_BLOCK), KV_BLOCK)
        out = []
        for g in range(group):
            w = jnp.exp(s_ref[g, :, cols] - maxes[g])
            s_ref[g, :, cols] = w
            acc = accs[g]
            for sl in lanes:
                acc = acc + w[:, sl]
            out.append(acc)
        return tuple(out)

    sums = lax.fori_loop(0, n_blocks, exp_step, tuple(jnp.zeros((rows, 128), jnp.float32) for _ in range(group)))
    invs = [1.0 / jnp.sum(a, axis=1, keepdims=True) for a in sums]

    def out_step(j, accs):
        cols = pl.ds(pl.multiple_of(j * KV_BLOCK, KV_BLOCK), KV_BLOCK)
        v_blk = v_ref[cols, :]
        return tuple(accs[g] + jnp.dot((s_ref[g, :, cols] * invs[g]).astype(jnp.bfloat16), v_blk,
                                       preferred_element_type=jnp.float32) for g in range(group))

    outs = lax.fori_loop(0, n_blocks, out_step, tuple(jnp.zeros((rows, HEAD_DIM), jnp.float32) for _ in range(group)))
    for g in range(group):
        o_ref[:, g * HEAD_DIM:(g + 1) * HEAD_DIM] = outs[g].astype(jnp.bfloat16)


def attention(q_rows, k_all, v_all, seg_q, seg_all, row_offset, row_stride, rows, block_rows):
    tokens = k_all.shape[0]
    width = q_rows.shape[1]
    group = width // HEAD_DIM
    steps = q_rows.shape[0] // rows
    return pl.pallas_call(
        functools.partial(attention_kernel, row_offset, row_stride, block_rows // rows, group),
        grid=(steps,),
        in_specs=[pl.BlockSpec((rows, width), lambda i: (i, 0)),
                  pl.BlockSpec((tokens, HEAD_DIM), lambda i: (0, 0)),
                  pl.BlockSpec((tokens, HEAD_DIM), lambda i: (0, 0)),
                  pl.BlockSpec((rows, 1), lambda i: (i, 0)),
                  pl.BlockSpec((1, tokens), lambda i: (0, 0))],
        out_specs=pl.BlockSpec((rows, width), lambda i: (i, 0)),
        out_shape=jax.ShapeDtypeStruct(q_rows.shape, jnp.bfloat16),
        scratch_shapes=[pltpu.VMEM((group, rows, tokens), jnp.float32)],
        compiler_params=pltpu.CompilerParams(vmem_limit_bytes=48 * 1024 * 1024),
        cost_estimate=pl.CostEstimate(flops=32 * q_rows.shape[0] * tokens * width, bytes_accessed=4 * tokens * HEAD_DIM,
                                      transcendentals=q_rows.shape[0] * tokens * group // 2),
    )(q_rows, k_all, v_all, seg_q, seg_all)


def solution(mesh):
    sp_size = mesh.shape["sp"]
    tp_size = mesh.shape["tp"]
    rep_size = mesh.shape["rep"]
    row_spec = P(("rep", "sp"), None)
    tok_spec = P(("rep", "sp"))
    full_spec = P(None)
    col_spec = P(None, "tp")
    wrow_spec = P("tp", None)
    cache_spec = P("rep", ("tp", "sp"), None)
    to_inner = [(0, 1), (3, 2)]
    across = [(1, 2), (2, 1)]
    to_end = [(1, 0), (2, 3)]
    swap = to_inner + to_end

    def exchange(piece_of, sp_index):
        own = piece_of(sp_index)
        parts = [own]
        for k in range(1, sp_size):
            parts.append(lax.ppermute(piece_of(sp_index ^ k), "sp", [(s, s ^ k) for s in range(sp_size)]))
        return parts

    def in_order(parts, sp_index, axis):
        return jnp.concatenate([lax.select_n(sp_index, *[parts[s ^ j] for s in range(sp_size)])
                                for j in range(sp_size)], axis=axis)

    def join_tp(from_low, from_high, tp_index):
        slabs = [lax.select_n(tp_index, *[from_low[p - j] if p >= j else from_high[j - p] for p in range(tp_size)])
                 for j in range(tp_size)]
        width = slabs[0].shape[1] // rep_size
        return jnp.concatenate([slab[:, r * width:(r + 1) * width] for r in range(rep_size) for slab in slabs], axis=1)

    def local_layer(x_in, positions, segments, gain_attn, w_q, w_k, w_v, w_o, gain_mlp, w_gate, w_up, w_down):
        rows_local, model_dim = x_in.shape
        sp_index = lax.axis_index("sp")
        tp_index = lax.axis_index("tp")
        rep_index = lax.axis_index("rep")
        is_low = tp_index < 2
        is_end = (tp_index == 0) | (tp_index == tp_size - 1)

        wo_rows = w_o.shape[0] // (rep_size * sp_size)
        wo_piece = lax.dynamic_slice_in_dim(w_o, (rep_index * sp_size + sp_index) * wo_rows, wo_rows, 0)
        wo_all = lax.all_gather(wo_piece, ("rep", "tp", "sp"), axis=0, tiled=True)

        x_f32 = x_in.astype(jnp.float32)
        u_norm = rms_norm(x_f32, gain_attn)
        cos_t, sin_t = rope_tables(positions)
        seg_all = in_order(exchange(lambda t: segments.reshape(-1, HEAD_DIM), sp_index), sp_index, 0).reshape(-1)
        k_rot = rotate_heads(jnp.dot(u_norm, w_k, preferred_element_type=jnp.float32), cos_t, sin_t)
        v_proj = jnp.dot(u_norm, w_v, preferred_element_type=jnp.float32).astype(jnp.bfloat16)
        kv_width = w_k.shape[1] // sp_size
        kv_parts = exchange(lambda t: jnp.concatenate(
            [lax.dynamic_slice_in_dim(k_rot, t * kv_width, kv_width, 1),
             lax.dynamic_slice_in_dim(v_proj, t * kv_width, kv_width, 1)], axis=1), sp_index)
        q_rot = rotate_heads(jnp.dot(u_norm, w_q, preferred_element_type=jnp.float32), cos_t, sin_t)
        q_width = w_q.shape[1] // sp_size
        q_parts = exchange(lambda t: lax.dynamic_slice_in_dim(q_rot, t * q_width, q_width, 1), sp_index)
        kv_all = in_order(kv_parts, sp_index, 0)
        k_all = kv_all[:, :kv_width]
        v_all = kv_all[:, kv_width:]
        q_all = in_order(q_parts, sp_index, 0).reshape(sp_size, rows_local, q_width)
        seg_blocks = seg_all.reshape(sp_size, rows_local)

        def attend(row_start, rows):
            q_rows = q_all[:, row_start:row_start + rows].reshape(sp_size * rows, q_width)
            seg_q = seg_blocks[:, row_start:row_start + rows].reshape(sp_size * rows, 1)
            return attention(q_rows, k_all, v_all, seg_q, seg_all[None, :], row_start, rows_local, ATTN_ROWS, rows)

        def attn_piece(attn, k):
            rows = attn.shape[0] // sp_size
            return lax.dynamic_slice_in_dim(attn, (sp_index ^ k) * rows, rows, 0)

        def sp_sends(attn):
            return [(attn_piece(attn, k), "sp", [(s, s ^ k) for s in range(sp_size)]) for k in range(1, sp_size)]

        def tp_sends(low, high, k):
            return [(low, "tp", [(i, i + 1) for i in range(k - 1, tp_size - 1)]),
                    (high, "tp", [(i + 1, i) for i in range(0, tp_size - k)])]

        def permute_all(sends):
            return [lax.ppermute(v, axis, perm) for v, axis, perm in sends]

        first_rows, later_rows = CHUNKS
        attn_first = attend(0, first_rows)
        attn_later = attend(first_rows, later_rows)
        recvs, attn_later = lax.optimization_barrier((permute_all(sp_sends(attn_first)), attn_later))
        own = in_order([attn_piece(attn_first, 0)] + recvs, sp_index, 1)
        from_low, from_high = [own], [own]
        for k in range(1, tp_size):
            low, high = permute_all(tp_sends(from_low[-1], from_high[-1], k))
            from_low.append(low)
            from_high.append(high)
        full_first = join_tp(from_low, from_high, tp_index)
        later_low, later_high = [], []

        def later_sends(t):
            if t == 0:
                return sp_sends(attn_later)
            if t < tp_size:
                return tp_sends(later_low[-1], later_high[-1], t)
            return []

        def later_landed(t, recvs):
            if t == 0:
                later_own = in_order([attn_piece(attn_later, 0)] + recvs, sp_index, 1)
                later_low.append(later_own)
                later_high.append(later_own)
            elif t < tp_size:
                later_low.append(recvs[0])
                later_high.append(recvs[1])

        def output_sum(row_start, attn_full):
            return x_in[row_start:row_start + attn_full.shape[0]].astype(jnp.float32) + jnp.dot(
                attn_full, wo_all, preferred_element_type=jnp.float32)

        def mlp_gate(x_mid):
            u_mlp = rms_norm(x_mid, gain_mlp)
            return u_mlp, jnp.dot(u_mlp, w_gate, preferred_element_type=jnp.float32)

        def mlp_hidden(u_mlp, gate_act):
            up_act = jnp.dot(u_mlp, w_up, preferred_element_type=jnp.float32)
            return (jax.nn.silu(gate_act) * up_act).astype(jnp.bfloat16)

        def mlp_down(hidden):
            return jnp.dot(hidden, w_down, preferred_element_type=jnp.float32)

        pieces = []
        landed = {}
        y_parts = []

        def add_pieces(row_start, rows, x_mid, partial, slot):
            half = rows // 2
            near = jnp.where(is_low, 0, half)
            for off in range(0, half, SUB_ROWS):
                take = lambda t, base, off=off: lax.dynamic_slice_in_dim(t, base + off, SUB_ROWS, 0)
                pieces.append(dict(slot=slot, p_near=lambda near=near, take=take: take(partial, near),
                                   p_far=lambda near=near, take=take: take(partial, half - near),
                                   x_near=lambda near=near, take=take: take(x_mid, near),
                                   row_near=row_start + near + off, row_far=row_start + half - near + off))
                slot += 1

        def sends_of(t):
            sends = []
            for i, pc in enumerate(pieces):
                stage = t - pc["slot"]
                if stage == 0:
                    sends.append((i, "sum_1", pc["p_far"](), to_inner))
                elif stage == 1:
                    sends.append((i, "sum_2", pc["p_far"]() + landed[i, "sum_1"], across))
                elif stage == 2:
                    sends.append((i, "sum_3", pc["p_near"]() + landed[i, "sum_2"], to_end))
                elif stage == 3:
                    y_end = (pc["x_near"]() + (pc["p_near"]() + landed[i, "sum_3"])).astype(jnp.bfloat16)
                    landed[i, "y_end"] = y_end
                    sends.append((i, "y_inner", y_end, to_inner))
                elif stage == 4:
                    y_near = jnp.where(is_end, landed[i, "y_end"], landed[i, "y_inner"])
                    y_parts.append((pc["row_near"], y_near))
                    sends.append((i, "y_cross", y_near, across))
                elif stage == 5:
                    sends.append((i, "y_back", landed[i, "y_cross"], to_end))
                elif stage == 6:
                    y_parts.append((pc["row_far"], jnp.where(is_end, landed[i, "y_back"], landed[i, "y_cross"])))
            return sends

        def merged(sends):
            groups = []
            for i, name, value, perm in sends:
                mate = [g for g in groups if perm is not across and g[2] is not across and g[2] is not perm
                        and g[1].dtype == value.dtype and len(g[0]) == 1]
                if mate:
                    inner, outer = (value, mate[0][1]) if perm is to_inner else (mate[0][1], value)
                    mate[0][:] = [mate[0][0] + [(i, name)], jnp.where(is_end, inner, outer), swap]
                else:
                    groups.append([[(i, name)], value, perm])
            return groups

        def run_slot(t, filler, *operands):
            sends = merged(sends_of(t))
            extra = later_sends(t)
            moved = [v for _, v, _ in sends] + [v for v, _, _ in extra]
            moved, operands = lax.optimization_barrier((moved, operands))
            routes = [("tp", perm) for _, _, perm in sends] + [(axis, perm) for _, axis, perm in extra]
            recvs = [lax.ppermute(v, axis, perm) for v, (axis, perm) in zip(moved, routes)]
            result = filler(*operands) if filler else ()
            recvs, result = lax.optimization_barrier((recvs, result))
            for (names, _, _), r in zip(sends, recvs):
                for key in names:
                    landed[key] = r
            later_landed(t, recvs[len(sends):])
            return result

        slot = 0
        row_start = 0
        for rows in CHUNKS:
            attn_full = full_first if slot == 0 else join_tp(later_low, later_high, tp_index)
            x_mid = run_slot(slot, lambda a: output_sum(row_start, a), attn_full)
            u_mlp, gate_act = run_slot(slot + 1, mlp_gate, x_mid)
            hidden = run_slot(slot + 2, mlp_hidden, u_mlp, gate_act)
            partial = run_slot(slot + 3, mlp_down, hidden)
            slot += 4
            add_pieces(row_start, rows, x_mid, partial, slot)
            row_start += rows
        while slot <= pieces[-1]["slot"] + 6:
            run_slot(slot, None)
            slot += 1
        y_out = jnp.zeros((rows_local, model_dim), jnp.bfloat16)
        for start, block in y_parts:
            y_out = lax.dynamic_update_slice_in_dim(y_out, block, start, 0)
        return y_out, k_all.reshape(-1, 1, HEAD_DIM), v_all.reshape(-1, 1, HEAD_DIM)

    return jax.shard_map(local_layer, mesh=mesh,
                         in_specs=(row_spec, tok_spec, tok_spec, full_spec, col_spec, col_spec, col_spec, wrow_spec,
                                   full_spec, col_spec, col_spec, wrow_spec),
                         out_specs=(row_spec, cache_spec, cache_spec), check_vma=False)
```

```python
import functools
import jax
import jax.numpy as jnp
from jax import lax
from jax.experimental import pallas as pl
from jax.experimental.pallas import tpu as pltpu
from jax.sharding import PartitionSpec as P

HEAD_DIM = 128
ROPE_BASE = 500000.0
NORM_EPS = 1e-5
CHUNKS = (512, 512)
ATTN_ROWS = 256
SUB_ROWS = 64
KV_BLOCK = 512
GATED_TILE = 256
WIDE_TILE = 768


def rms_norm(x_f32, gain_vec):
    mean_sq = jnp.mean(x_f32 * x_f32, axis=-1, keepdims=True)
    return (x_f32 * lax.rsqrt(mean_sq + NORM_EPS) * gain_vec).astype(jnp.bfloat16)


def rope_tables(positions):
    half_dim = HEAD_DIM // 2
    inv_freq = jnp.power(jnp.float32(ROPE_BASE), -jnp.arange(half_dim, dtype=jnp.float32) * (2.0 / HEAD_DIM))
    angles = positions.astype(jnp.float32)[:, None] * inv_freq
    return jnp.cos(angles), jnp.sin(angles)


def rotate_heads(t_f32, cos_t, sin_t):
    half_dim = HEAD_DIM // 2
    pieces = []
    for start in range(0, t_f32.shape[1], HEAD_DIM):
        t_lo = t_f32[:, start:start + half_dim]
        t_hi = t_f32[:, start + half_dim:start + HEAD_DIM]
        pieces += [t_lo * cos_t - t_hi * sin_t, t_hi * cos_t + t_lo * sin_t]
    return jnp.concatenate(pieces, axis=1).astype(jnp.bfloat16)


def attention_kernel(row_offset, row_stride, per_block, group, q_ref, k_ref, v_ref, segq_ref, segk_ref, o_ref, s_ref):
    rows = q_ref.shape[0]
    row_start = lax.div(pl.program_id(0), per_block) * row_stride + row_offset + lax.rem(pl.program_id(0), per_block) * rows
    n_blocks = lax.div(row_start + rows + KV_BLOCK - 1, KV_BLOCK)
    seg_q = segq_ref[...]
    row_ids = row_start + lax.broadcasted_iota(jnp.int32, (rows, KV_BLOCK), 0)
    lane_ids = lax.broadcasted_iota(jnp.int32, (rows, KV_BLOCK), 1)
    lanes = [slice(i, i + 128) for i in range(0, KV_BLOCK, 128)]

    def score_step(j, accs):
        cols = pl.ds(pl.multiple_of(j * KV_BLOCK, KV_BLOCK), KV_BLOCK)
        k_blk = k_ref[cols, :]
        allowed = (row_ids >= lane_ids + j * KV_BLOCK) & (seg_q == segk_ref[:, cols])
        out = []
        for g in range(group):
            scores = lax.dot_general(q_ref[:, g * HEAD_DIM:(g + 1) * HEAD_DIM], k_blk, (((1,), (1,)), ((), ())),
                                     preferred_element_type=jnp.float32) * (HEAD_DIM ** -0.5)
            scores = jnp.where(allowed, scores, -1e30)
            s_ref[g, :, cols] = scores
            acc = accs[g]
            for sl in lanes:
                acc = jnp.maximum(acc, scores[:, sl])
            out.append(acc)
        return tuple(out)

    accs = lax.fori_loop(0, n_blocks, score_step, tuple(jnp.full((rows, 128), -1e30, jnp.float32) for _ in range(group)))
    maxes = [jnp.max(a, axis=1, keepdims=True) for a in accs]

    def exp_step(j, accs):
        cols = pl.ds(pl.multiple_of(j * KV_BLOCK, KV_BLOCK), KV_BLOCK)
        out = []
        for g in range(group):
            w = jnp.exp(s_ref[g, :, cols] - maxes[g])
            s_ref[g, :, cols] = w
            acc = accs[g]
            for sl in lanes:
                acc = acc + w[:, sl]
            out.append(acc)
        return tuple(out)

    sums = lax.fori_loop(0, n_blocks, exp_step, tuple(jnp.zeros((rows, 128), jnp.float32) for _ in range(group)))
    invs = [1.0 / jnp.sum(a, axis=1, keepdims=True) for a in sums]

    def out_step(j, accs):
        cols = pl.ds(pl.multiple_of(j * KV_BLOCK, KV_BLOCK), KV_BLOCK)
        v_blk = v_ref[cols, :]
        return tuple(accs[g] + jnp.dot((s_ref[g, :, cols] * invs[g]).astype(jnp.bfloat16), v_blk,
                                       preferred_element_type=jnp.float32) for g in range(group))

    outs = lax.fori_loop(0, n_blocks, out_step, tuple(jnp.zeros((rows, HEAD_DIM), jnp.float32) for _ in range(group)))
    for g in range(group):
        o_ref[:, g * HEAD_DIM:(g + 1) * HEAD_DIM] = outs[g].astype(jnp.bfloat16)


def attention(q_rows, k_all, v_all, seg_q, seg_all, row_offset, row_stride, rows, block_rows):
    tokens = k_all.shape[0]
    width = q_rows.shape[1]
    group = width // HEAD_DIM
    steps = q_rows.shape[0] // rows
    return pl.pallas_call(
        functools.partial(attention_kernel, row_offset, row_stride, block_rows // rows, group),
        grid=(steps,),
        in_specs=[pl.BlockSpec((rows, width), lambda i: (i, 0)),
                  pl.BlockSpec((tokens, HEAD_DIM), lambda i: (0, 0)),
                  pl.BlockSpec((tokens, HEAD_DIM), lambda i: (0, 0)),
                  pl.BlockSpec((rows, 1), lambda i: (i, 0)),
                  pl.BlockSpec((1, tokens), lambda i: (0, 0))],
        out_specs=pl.BlockSpec((rows, width), lambda i: (i, 0)),
        out_shape=jax.ShapeDtypeStruct(q_rows.shape, jnp.bfloat16),
        scratch_shapes=[pltpu.VMEM((group, rows, tokens), jnp.float32)],
        compiler_params=pltpu.CompilerParams(vmem_limit_bytes=48 * 1024 * 1024),
        cost_estimate=pl.CostEstimate(flops=32 * q_rows.shape[0] * tokens * width, bytes_accessed=4 * tokens * HEAD_DIM,
                                      transcendentals=q_rows.shape[0] * tokens * group // 2),
    )(q_rows, k_all, v_all, seg_q, seg_all)


def dot_f32(a, b):
    return jnp.dot(a, b, preferred_element_type=jnp.float32)


def residual_kernel(a_ref, w_ref, x_ref, o_ref):
    o_ref[...] = x_ref[...].astype(jnp.float32) + dot_f32(a_ref[...], w_ref[...])


def gated_kernel(u_ref, wg_ref, wu_ref, o_ref):
    gate_act = dot_f32(u_ref[...], wg_ref[...])
    up_act = dot_f32(u_ref[...], wu_ref[...])
    o_ref[...] = (jax.nn.silu(gate_act) * up_act).astype(o_ref.dtype)


def down_kernel(a_ref, b_ref, w_ref, o_ref):
    mid = a_ref.shape[1]
    o_ref[...] = dot_f32(a_ref[...], w_ref[:mid, :]) + dot_f32(b_ref[...], w_ref[mid:, :])


def column_call(kernel, whole, tiled, out_cols, out_dtype, tile, first_tile=0):
    rows = whole[0].shape[0]
    flops = 2 * rows * out_cols * sum(w.shape[0] for w in tiled if w.shape[0] != rows)
    return pl.pallas_call(
        kernel,
        grid=(out_cols // tile,),
        in_specs=[pl.BlockSpec(a.shape, lambda i: (0, 0)) for a in whole]
        + [pl.BlockSpec((w.shape[0], tile), lambda i: (0, i + first_tile)) for w in tiled],
        out_specs=pl.BlockSpec((rows, tile), lambda i: (0, i)),
        out_shape=jax.ShapeDtypeStruct((rows, out_cols), out_dtype),
        compiler_params=pltpu.CompilerParams(vmem_limit_bytes=60 * 1024 * 1024),
        cost_estimate=pl.CostEstimate(flops=flops, bytes_accessed=flops // rows, transcendentals=0),
    )(*whole, *tiled)


def solution(mesh):
    sp_size = mesh.shape["sp"]
    tp_size = mesh.shape["tp"]
    rep_size = mesh.shape["rep"]
    row_spec = P(("rep", "sp"), None)
    tok_spec = P(("rep", "sp"))
    full_spec = P(None)
    col_spec = P(None, "tp")
    wrow_spec = P("tp", None)
    cache_spec = P("rep", ("tp", "sp"), None)
    to_inner = [(0, 1), (3, 2)]
    across = [(1, 2), (2, 1)]
    to_end = [(1, 0), (2, 3)]
    swap = to_inner + to_end

    def exchange(piece_of, sp_index):
        own = piece_of(sp_index)
        parts = [own]
        for k in range(1, sp_size):
            parts.append(lax.ppermute(piece_of(sp_index ^ k), "sp", [(s, s ^ k) for s in range(sp_size)]))
        return parts

    def in_order(parts, sp_index, axis):
        return jnp.concatenate([lax.select_n(sp_index, *[parts[s ^ j] for s in range(sp_size)])
                                for j in range(sp_size)], axis=axis)

    def join_tp(from_low, from_high, tp_index):
        slabs = [lax.select_n(tp_index, *[from_low[p - j] if p >= j else from_high[j - p] for p in range(tp_size)])
                 for j in range(tp_size)]
        width = slabs[0].shape[1] // rep_size
        return jnp.concatenate([slab[:, r * width:(r + 1) * width] for r in range(rep_size) for slab in slabs], axis=1)

    def local_layer(x_in, positions, segments, gain_attn, w_q, w_k, w_v, w_o, gain_mlp, w_gate, w_up, w_down):
        rows_local, model_dim = x_in.shape
        sp_index = lax.axis_index("sp")
        tp_index = lax.axis_index("tp")
        rep_index = lax.axis_index("rep")
        is_low = tp_index < 2
        is_end = (tp_index == 0) | (tp_index == tp_size - 1)

        wo_rows = w_o.shape[0] // (rep_size * sp_size)
        wo_piece = lax.dynamic_slice_in_dim(w_o, (rep_index * sp_size + sp_index) * wo_rows, wo_rows, 0)
        wo_all = lax.all_gather(wo_piece, ("rep", "tp", "sp"), axis=0, tiled=True)

        x_f32 = x_in.astype(jnp.float32)
        u_norm = rms_norm(x_f32, gain_attn)
        cos_t, sin_t = rope_tables(positions)
        seg_all = in_order(exchange(lambda t: segments.reshape(-1, HEAD_DIM), sp_index), sp_index, 0).reshape(-1)
        k_rot = rotate_heads(jnp.dot(u_norm, w_k, preferred_element_type=jnp.float32), cos_t, sin_t)
        v_proj = jnp.dot(u_norm, w_v, preferred_element_type=jnp.float32).astype(jnp.bfloat16)
        kv_width = w_k.shape[1] // sp_size
        kv_parts = exchange(lambda t: jnp.concatenate(
            [lax.dynamic_slice_in_dim(k_rot, t * kv_width, kv_width, 1),
             lax.dynamic_slice_in_dim(v_proj, t * kv_width, kv_width, 1)], axis=1), sp_index)
        q_rot = rotate_heads(jnp.dot(u_norm, w_q, preferred_element_type=jnp.float32), cos_t, sin_t)
        q_width = w_q.shape[1] // sp_size
        q_parts = exchange(lambda t: lax.dynamic_slice_in_dim(q_rot, t * q_width, q_width, 1), sp_index)
        kv_all = in_order(kv_parts, sp_index, 0)
        k_all = kv_all[:, :kv_width]
        v_all = kv_all[:, kv_width:]
        q_all = in_order(q_parts, sp_index, 0).reshape(sp_size, rows_local, q_width)
        seg_blocks = seg_all.reshape(sp_size, rows_local)

        def attend(row_start, rows):
            q_rows = q_all[:, row_start:row_start + rows].reshape(sp_size * rows, q_width)
            seg_q = seg_blocks[:, row_start:row_start + rows].reshape(sp_size * rows, 1)
            return attention(q_rows, k_all, v_all, seg_q, seg_all[None, :], row_start, rows_local, ATTN_ROWS, rows)

        def attn_piece(attn, k):
            rows = attn.shape[0] // sp_size
            return lax.dynamic_slice_in_dim(attn, (sp_index ^ k) * rows, rows, 0)

        def sp_sends(attn):
            return [(attn_piece(attn, k), "sp", [(s, s ^ k) for s in range(sp_size)]) for k in range(1, sp_size)]

        def tp_sends(low, high, k):
            return [(low, "tp", [(i, i + 1) for i in range(k - 1, tp_size - 1)]),
                    (high, "tp", [(i + 1, i) for i in range(0, tp_size - k)])]

        def permute_all(sends):
            return [lax.ppermute(v, axis, perm) for v, axis, perm in sends]

        first_rows, later_rows = CHUNKS
        attn_first = attend(0, first_rows)
        attn_later = attend(first_rows, later_rows)
        recvs, attn_later = lax.optimization_barrier((permute_all(sp_sends(attn_first)), attn_later))
        own = in_order([attn_piece(attn_first, 0)] + recvs, sp_index, 1)
        from_low, from_high = [own], [own]
        for k in range(1, tp_size):
            low, high = permute_all(tp_sends(from_low[-1], from_high[-1], k))
            from_low.append(low)
            from_high.append(high)
        full_first = join_tp(from_low, from_high, tp_index)
        later_low, later_high = [], []

        def later_sends(t):
            if t == 0:
                return sp_sends(attn_later)
            if t < tp_size:
                return tp_sends(later_low[-1], later_high[-1], t)
            return []

        def later_landed(t, recvs):
            if t == 0:
                later_own = in_order([attn_piece(attn_later, 0)] + recvs, sp_index, 1)
                later_low.append(later_own)
                later_high.append(later_own)
            elif t < tp_size:
                later_low.append(recvs[0])
                later_high.append(recvs[1])

        def output_sum(row_start, attn_full):
            return column_call(residual_kernel, [attn_full], [wo_all, x_in[row_start:row_start + attn_full.shape[0]]],
                               model_dim, jnp.float32, WIDE_TILE)

        ff_tiles = w_gate.shape[1] // GATED_TILE
        front_tiles = (ff_tiles + 1) // 2

        def mlp_front(x_mid):
            u_mlp = rms_norm(x_mid, gain_mlp)
            return u_mlp, column_call(gated_kernel, [u_mlp], [w_gate, w_up],
                                      front_tiles * GATED_TILE, jnp.bfloat16, GATED_TILE)

        def mlp_back(u_mlp, hidden_front):
            return hidden_front, column_call(gated_kernel, [u_mlp], [w_gate, w_up],
                                             (ff_tiles - front_tiles) * GATED_TILE, jnp.bfloat16, GATED_TILE, front_tiles)

        def mlp_down(hidden_front, hidden_back):
            return column_call(down_kernel, [hidden_front, hidden_back], [w_down], model_dim, jnp.float32, WIDE_TILE)

        pieces = []
        landed = {}
        y_parts = []

        def add_pieces(row_start, rows, x_mid, partial, slot):
            half = rows // 2
            near = jnp.where(is_low, 0, half)
            for off in range(0, half, SUB_ROWS):
                take = lambda t, base, off=off: lax.dynamic_slice_in_dim(t, base + off, SUB_ROWS, 0)
                pieces.append(dict(slot=slot, p_near=lambda near=near, take=take: take(partial, near),
                                   p_far=lambda near=near, take=take: take(partial, half - near),
                                   x_near=lambda near=near, take=take: take(x_mid, near),
                                   row_near=row_start + near + off, row_far=row_start + half - near + off))
                slot += 1

        def sends_of(t):
            sends = []
            for i, pc in enumerate(pieces):
                stage = t - pc["slot"]
                if stage == 0:
                    sends.append((i, "sum_1", pc["p_far"](), to_inner))
                elif stage == 1:
                    sends.append((i, "sum_2", pc["p_far"]() + landed[i, "sum_1"], across))
                elif stage == 2:
                    sends.append((i, "sum_3", pc["p_near"]() + landed[i, "sum_2"], to_end))
                elif stage == 3:
                    y_end = (pc["x_near"]() + (pc["p_near"]() + landed[i, "sum_3"])).astype(jnp.bfloat16)
                    landed[i, "y_end"] = y_end
                    sends.append((i, "y_inner", y_end, to_inner))
                elif stage == 4:
                    y_near = jnp.where(is_end, landed[i, "y_end"], landed[i, "y_inner"])
                    y_parts.append((pc["row_near"], y_near))
                    sends.append((i, "y_cross", y_near, across))
                elif stage == 5:
                    sends.append((i, "y_back", landed[i, "y_cross"], to_end))
                elif stage == 6:
                    y_parts.append((pc["row_far"], jnp.where(is_end, landed[i, "y_back"], landed[i, "y_cross"])))
            return sends

        def merged(sends):
            groups = []
            for i, name, value, perm in sends:
                mate = [g for g in groups if perm is not across and g[2] is not across and g[2] is not perm
                        and g[1].dtype == value.dtype and len(g[0]) == 1]
                if mate:
                    inner, outer = (value, mate[0][1]) if perm is to_inner else (mate[0][1], value)
                    mate[0][:] = [mate[0][0] + [(i, name)], jnp.where(is_end, inner, outer), swap]
                else:
                    groups.append([[(i, name)], value, perm])
            return groups

        def run_slot(t, filler, *operands):
            sends = merged(sends_of(t))
            extra = later_sends(t)
            moved = [v for _, v, _ in sends] + [v for v, _, _ in extra]
            moved, operands = lax.optimization_barrier((moved, operands))
            routes = [("tp", perm) for _, _, perm in sends] + [(axis, perm) for _, axis, perm in extra]
            recvs = [lax.ppermute(v, axis, perm) for v, (axis, perm) in zip(moved, routes)]
            result = filler(*operands) if filler else ()
            recvs, result = lax.optimization_barrier((recvs, result))
            for (names, _, _), r in zip(sends, recvs):
                for key in names:
                    landed[key] = r
            later_landed(t, recvs[len(sends):])
            return result

        slot = 0
        row_start = 0
        for rows in CHUNKS:
            attn_full = full_first if slot == 0 else join_tp(later_low, later_high, tp_index)
            x_mid = run_slot(slot, lambda a: output_sum(row_start, a), attn_full)
            u_mlp, hidden_front = run_slot(slot + 1, mlp_front, x_mid)
            hidden = run_slot(slot + 2, mlp_back, u_mlp, hidden_front)
            partial = run_slot(slot + 3, mlp_down, *hidden)
            slot += 4
            add_pieces(row_start, rows, x_mid, partial, slot)
            row_start += rows
        while slot <= pieces[-1]["slot"] + 6:
            run_slot(slot, None)
            slot += 1
        y_out = jnp.zeros((rows_local, model_dim), jnp.bfloat16)
        for start, block in y_parts:
            y_out = lax.dynamic_update_slice_in_dim(y_out, block, start, 0)
        return y_out, k_all.reshape(-1, 1, HEAD_DIM), v_all.reshape(-1, 1, HEAD_DIM)

    return jax.shard_map(local_layer, mesh=mesh,
                         in_specs=(row_spec, tok_spec, tok_spec, full_spec, col_spec, col_spec, col_spec, wrow_spec,
                                   full_spec, col_spec, col_spec, wrow_spec),
                         out_specs=(row_spec, cache_spec, cache_spec), check_vma=False)
```
